32 devices in a mesh: dp: 4 (over x, core), row: 2 (over y), col: 4 (over z).
Axes of the slice: x: 2, y: 2, z: 4, core: 2. Of those that a mesh axis runs over, the one named last changes fastest.
Arguments:
- act_in: bfloat16 [4096, 2304], P(('dp', 'row'), 'col'), may hold values from -6 to 6
- cot_out: bfloat16 [4096, 2304], P(('dp', 'row'), 'col'), may hold values from -6 to 6
- w_gate: bfloat16 [2304, 4608], P(('dp', 'row'), 'col'), may hold values from -0.125 to 0.125
- w_up: bfloat16 [2304, 4608], P(('dp', 'row'), 'col'), may hold values from -0.125 to 0.125
- w_down: bfloat16 [4608, 2304], P('col', ('dp', 'row')), may hold values from -0.09375 to 0.09375
Outputs:
- input_grad: bfloat16 [4096, 2304], P(('dp', 'row'), 'col')
- gate_grad: float32 [2304, 4608], P(('dp', 'row'), 'col')
- up_grad: float32 [2304, 4608], P(('dp', 'row'), 'col')
- down_grad: float32 [4608, 2304], P('col', ('dp', 'row'))
The draws below stay inside these ranges and needn't reach their ends.
All inputs are finite; a program needn't handle non-finite values.
Results may differ from the reference program's by a relative error of at most 0.015.
Values may be sent and summed in bfloat16 or wider, within the bound.
A program may use at most 128 MiB of HBM per device.

```python
import math
import jax
import jax.numpy as jnp
from jax import lax

D = 2304
FF = 4608
TOKENS = 4096
N_COL = 4


def with_spikes(result, key, source, target, shards_of, factor):
    def block_of(position):
        return (jnp.arange(result.shape[position]) // (result.shape[position] // shards_of)).reshape((-1,) + (1,) * (result.ndim - 1 - position))

    near = jax.random.permutation(key, shards_of)[block_of(target)]
    second = (block_of(target) + shards_of // 2) % shards_of
    return jnp.where((block_of(source) == near) | (block_of(source) == second), factor * result, result)


def levels(stream_key, dims, split, smallest, largest):
    loudness, own = 1.0, jax.random.fold_in(stream_key, 6)
    for dim, blocks in split:
        heights = jnp.exp(jax.random.uniform(jax.random.fold_in(own, dim), (blocks,), jnp.float32, smallest / len(split), largest / len(split)))
        loudness = loudness * jnp.repeat(heights, dims[dim] // blocks).reshape([-1 if axis == dim else 1 for axis in range(len(dims))])
    return loudness


def gaussian(rng, extent, deviation, reach, pieces=(), held_as=jnp.bfloat16):
    array = deviation * jax.random.normal(rng, extent, jnp.float32)
    if pieces:
        array = array * levels(rng, extent, pieces, -0.22, 0.18)
    return jnp.clip(array, -reach, reach).astype(held_as)


def heavy_noise(rng, extent, spread, bound, cuts, heavy, dtype=jnp.bfloat16):
    values = spread * jax.random.normal(rng, extent, jnp.float32)
    if cuts:
        values = values * levels(rng, extent, cuts, -0.22, 0.18)
    return jnp.clip(with_spikes(values, jax.random.fold_in(rng, 3), *heavy), -bound, bound).astype(dtype)


def setup_inputs(seed: int = 0) -> dict:
    splits = jax.random.split(jax.random.key(seed), 6)
    act_in = heavy_noise(splits[0], (TOKENS, D), 1.0, 6.0, ((0, 8), (1, 4)), (0, 1, 8, 2.0))
    cot_out = heavy_noise(splits[1], (TOKENS, D), 1.0, 6.0, ((0, 8), (1, 4)), (0, 1, 8, 2.0))
    w_gate = gaussian(splits[2], (D, FF), D ** -0.5, 0.125, ((0, 8), (1, 4)))
    w_up = gaussian(splits[3], (D, FF), D ** -0.5, 0.125, ((0, 8), (1, 4)))
    w_down = gaussian(splits[4], (FF, D), FF ** -0.5, 0.09375, ((0, 4), (1, 8)))
    return {"act_in": act_in, "cot_out": cot_out, "w_gate": w_gate, "w_up": w_up, "w_down": w_down}


gelu_cubic = 0.044715
gelu_scale = 0.7978845608028654

def gelu_parts(values):
    inner_arg = gelu_scale * (values + gelu_cubic * values * values * values)
    tanh_val = jnp.tanh(inner_arg)
    output = 0.5 * values * (1.0 + tanh_val)
    slope_val = 0.5 * (1.0 + tanh_val) + 0.5 * values * (1.0 - tanh_val * tanh_val) * gelu_scale * (1.0 + 3.0 * gelu_cubic * values * values)
    return (output, slope_val)

def reference(act_in, cot_out, w_gate, w_up, w_down):
    gate_pre = jnp.dot(act_in, w_gate, preferred_element_type=jnp.float32)
    up_pre = jnp.dot(act_in, w_up, preferred_element_type=jnp.float32)
    act_val, slope_val = gelu_parts(gate_pre)
    hidden = (act_val * up_pre).astype(jnp.bfloat16)
    hidden_grad = jnp.dot(cot_out, w_down.T, preferred_element_type=jnp.float32)
    d_gate = (hidden_grad * up_pre * slope_val).astype(jnp.bfloat16)
    d_up = (hidden_grad * act_val).astype(jnp.bfloat16)
    width = FF // N_COL
    input_sum = jnp.zeros(act_in.shape, jnp.float32)
    for column in range(N_COL):
        low_edge = column * width
        part_sum = jnp.dot(d_gate[:, low_edge:low_edge + width], w_gate[:, low_edge:low_edge + width].T, preferred_element_type=jnp.float32)
        part_sum = part_sum + jnp.dot(d_up[:, low_edge:low_edge + width], w_up[:, low_edge:low_edge + width].T, preferred_element_type=jnp.float32)
        input_sum = input_sum + lax.optimization_barrier(part_sum.astype(jnp.bfloat16)).astype(jnp.float32)
    input_grad = input_sum.astype(jnp.bfloat16)
    norm_scale = 1.0 / math.sqrt(TOKENS)
    gate_grad = jnp.dot(act_in.T, d_gate, preferred_element_type=jnp.float32) * norm_scale
    up_grad = jnp.dot(act_in.T, d_up, preferred_element_type=jnp.float32) * norm_scale
    down_grad = jnp.dot(hidden.T, cot_out, preferred_element_type=jnp.float32) * norm_scale
    return (input_grad, gate_grad, up_grad, down_grad)
```

```python
import functools
import math

import jax
import jax.numpy as jnp
from jax import lax
from jax.experimental import pallas as pl
from jax.experimental.pallas import tpu as pltpu
from jax.sharding import PartitionSpec as P

gelu_cubic = 0.044715
gelu_scale = 0.7978845608028654
MESH = pl.DeviceIdType.MESH
F32 = jnp.float32
BF16 = jnp.bfloat16


def gelu_parts(values):
    inner_arg = gelu_scale * (values + gelu_cubic * values * values * values)
    tanh_val = jnp.tanh(inner_arg)
    output = 0.5 * values * (1.0 + tanh_val)
    slope_val = 0.5 * (1.0 + tanh_val) + 0.5 * values * (1.0 - tanh_val * tanh_val) * gelu_scale * (
        1.0 + 3.0 * gelu_cubic * values * values
    )
    return (output, slope_val)


def tile_of(size, best):
    return best if size % best == 0 else size


def pieces_of(rows):
    if rows % 32 == 0:
        return [(0, 0, rows, 0), (1, 0, rows, 1), (2, 0, rows // 2, 0), (2, rows // 2, rows // 2, 1)]
    return [(0, 0, rows, 0), (1, 0, rows, 1), (2, 0, rows, 0)]


def others_first(n):
    return list(range(1, n)) + [0]


class Sends:
    def __init__(self, sems):
        self.sems, self.used, self.pending = sems, 0, []

    def start(self, src, dst, recv_sem, where, cond=None):
        copy = pltpu.make_async_remote_copy(
            src_ref=src,
            dst_ref=dst,
            send_sem=self.sems.at[self.used],
            recv_sem=recv_sem,
            device_id=where,
            device_id_type=MESH,
        )
        self.used += 1
        self.pending.append((cond, copy))
        guarded(cond, copy.start)

    def finish(self):
        for cond, copy in self.pending:
            guarded(cond, copy.wait_send)


def guarded(cond, action):
    if cond is None:
        action()
    else:
        pl.when(cond)(action)


def arrived(ref, sem):
    pltpu.make_async_copy(ref, ref, sem).wait()


def kernel(sizes, act_ref, cot_ref, wg_ref, wu_ref, wd_ref, ig_ref, og_ref, ou_ref, od_ref,
           full, weights, grads, stash, acc, partner_out, sums, first_in, second_in, ig_out, ig_in, outs,
           own_sem, send_sem, w_sem, x_sem, pair_send, pair_recv, first_sem, second_sem, ig_sem, out_sem):
    n_dp, n_row, n_col, rows, hid, feats, toks = sizes
    nq, ny = n_dp // 2, n_row
    peers = nq * ny
    pieces = pieces_of(rows)
    dp, y, col = lax.axis_index("dp"), lax.axis_index("row"), lax.axis_index("col")
    q, c = dp // 2, dp % 2
    rep_of = lambda q1, c1, y1: (q1 * 2 + c1) * ny + y1
    at_q = lambda dq: lax.rem(q + dq, nq)
    at_y = lambda dy: lax.rem(y + dy, ny)
    back_q = lambda dq: lax.rem(q + nq - dq, nq)
    back_y = lambda dy: lax.rem(y + ny - dy, ny)
    me = rep_of(q, c, y)
    partner = {"dp": q * 2 + 1 - c}
    q_peer = lambda dq: {"dp": at_q(dq) * 2 + c}
    y_peer = lambda dy: {"row": at_y(dy)}
    xs, ys = [q_peer(i) for i in range(1, nq)], [y_peer(i) for i in range(1, ny)]

    barrier = pltpu.get_barrier_semaphore()
    friends = [partner] + xs + ys
    friends += [{"col": lax.rem(col + i, n_col)} for i in range(1, n_col)]
    for friend in friends:
        pl.semaphore_signal(barrier, inc=1, device_id=friend, device_id_type=MESH)
    pl.semaphore_wait(barrier, len(friends))

    sends = Sends(send_sem)
    mine = (wg_ref, wu_ref, wd_ref)
    streams = (act_ref, cot_ref)

    def rows_at(rep, r0, nr):
        return pl.ds(pl.multiple_of(rep * rows + r0, 8), nr)

    def slot(p, rep):
        w, r0, nr, _ = pieces[p]
        return weights.at[w, rows_at(rep, r0, nr), :]

    half = feats // 2

    def feat_slot(s, h, block):
        return full.at[s, pl.ds(pl.multiple_of(block * feats + h * half, 8), half), :]

    def feat_sem(s, h, block):
        return x_sem.at[(s * 2 + h) * n_col + block]

    has_right, has_left = col < n_col - 1, col > 0
    right = {"col": jnp.minimum(col + 1, n_col - 1)}
    left = {"col": jnp.maximum(col - 1, 0)}

    def own_features(s):
        for h in range(2):
            src = streams[s].at[pl.ds(h * half, half), :]
            sends.start(src, feat_slot(s, h, col), feat_sem(s, h, col), right, has_right)
            sends.start(src, feat_slot(s, h, col), feat_sem(s, h, col), left, has_left)

    def own_piece(p, wheres):
        w, r0, nr, _ = pieces[p]
        for where in wheres:
            sends.start(mine[w].at[pl.ds(r0, nr), :], slot(p, me), w_sem.at[p * peers * 2 + me], where)

    early = [p for p in range(len(pieces)) if pieces[p][0] < 2]
    later = [p for p in range(len(pieces)) if pieces[p][0] == 2]
    own_features(0)
    for p in early:
        own_piece(p, xs)
    for p in reversed(early):
        own_piece(p, ys)
    for p in early:
        own_piece(p, [partner])
    locals_ = []
    for i, (src, dst) in enumerate(
        [(streams[s], full.at[s, pl.ds(pl.multiple_of(col * feats, 8), feats), :]) for s in range(2)]
        + [(mine[w], weights.at[w, rows_at(me, 0, rows), :]) for w in range(3)]
    ):
        locals_.append(pltpu.make_async_copy(src, dst, own_sem.at[i]))
        locals_[-1].start()

    def chain(s, step):
        from_left, from_right = col >= step, col + step < n_col
        lb, rb = jnp.maximum(col - step, 0), jnp.minimum(col + step, n_col - 1)
        for h in range(2):
            l_slot, l_sem = feat_slot(s, h, lb), feat_sem(s, h, lb)
            r_slot, r_sem = feat_slot(s, h, rb), feat_sem(s, h, rb)
            guarded(from_left, lambda: arrived(l_slot, l_sem))
            if step < n_col - 1:
                sends.start(l_slot, l_slot, l_sem, right, from_left & has_right)
            guarded(from_right, lambda: arrived(r_slot, r_sem))
            if step < n_col - 1:
                sends.start(r_slot, r_slot, r_sem, left, from_right & has_left)

    def take(p, rep, forward):
        sem = w_sem.at[p * peers * 2 + rep]
        arrived(slot(p, rep), sem)
        for where in forward + [partner]:
            sends.start(slot(p, rep), slot(p, rep), sem, where)

    def near_first(p):
        if pieces[p][3] == 0:
            for dq in range(1, nq):
                take(p, rep_of(back_q(dq), c, y), ys)
        else:
            for dy in range(1, ny):
                take(p, rep_of(q, c, back_y(dy)), xs)

    def near_rest(p):
        if pieces[p][3] == 0:
            for dy in range(1, ny):
                take(p, rep_of(q, c, back_y(dy)), [])
        else:
            for dq in range(1, nq):
                take(p, rep_of(back_q(dq), c, y), [])

    def far(p):
        for dq in range(1, nq):
            for dy in range(1, ny):
                take(p, rep_of(back_q(dq), c, back_y(dy)), [])

    def from_partner(p):
        for dq in range(nq):
            for dy in range(ny):
                rep = rep_of(at_q(dq), 1 - c, at_y(dy))
                arrived(slot(p, rep), w_sem.at[p * peers * 2 + rep])

    chain(0, 1)
    for p in early:
        near_first(p)
    for p in later:
        own_piece(p, xs)
    for p in reversed(later):
        own_piece(p, ys)
    for p in later:
        own_piece(p, [partner])
    for step in range(2, n_col - 1):
        chain(0, step)
    own_features(1)
    for p in early:
        near_rest(p)
    if n_col > 2:
        chain(0, n_col - 1)
    chain(1, 1)
    for p in early:
        far(p)
    for p in early:
        from_partner(p)
    for copy in locals_:
        copy.wait()

    mt, nt = tile_of(toks, 256), tile_of(hid, 384)
    m_tiles, n_tiles = toks // mt, hid // nt
    token_dims = (((0,), (0,)), ((), ()))

    def tile_slices(i):
        m, n = i // n_tiles, i % n_tiles
        return pl.ds(pl.multiple_of(m * mt, mt), mt), pl.ds(pl.multiple_of(n * nt, nt), nt)

    def project(first, last):
        @pl.loop(first, last)
        def _(i):
            ms, ns = tile_slices(i)
            x = full[0, :, ms]
            gate_pre = lax.dot_general(x, weights[0, :, ns], token_dims, preferred_element_type=F32)
            up_pre = lax.dot_general(x, weights[1, :, ns], token_dims, preferred_element_type=F32)
            act_val, slope_val = gelu_parts(gate_pre)
            grads[2, ms, ns] = (act_val * up_pre).astype(BF16)
            stash[0, ms, ns] = up_pre * slope_val
            stash[1, ms, ns] = act_val

    tiles = m_tiles * n_tiles
    project(0, tiles // 2)
    for p in later:
        near_first(p)
    project(tiles // 2, tiles)

    def n_slice(n):
        return pl.ds(pl.multiple_of(n * nt, nt), nt)

    def term(w, rep, ns):
        return jnp.dot(full[w // 2, rows_at(rep, 0, rows), :], grads[w, :, ns], preferred_element_type=F32)

    def pair_copy(i):
        return pltpu.make_async_remote_copy(
            src_ref=partner_out.at[i],
            dst_ref=sums.at[i],
            send_sem=pair_send.at[i],
            recv_sem=pair_recv.at[i],
            device_id=partner,
            device_id_type=MESH,
        )

    def distance(rep):
        return jnp.abs((rep * rows) // feats - col)

    first_base, count = [], [0, 0]
    for w, _, _, route in pieces:
        first_base.append(count[w // 2])
        count[w // 2] += (nq - 1) * ny if route == 0 else (ny - 1) * nq
    second_base, count = [], [0, 0]
    for w, _, _, route in pieces:
        second_base.append(count[w // 2])
        count[w // 2] += (ny - 1) if route == 0 else (nq - 1)

    def first_slot(p, dq, dy):
        k = first_base[p] + ((dq - 1) * ny + dy if pieces[p][3] == 0 else (dy - 1) * nq + dq)
        late = pieces[p][0] // 2
        return first_in[late].at[k], first_sem[late].at[k]

    def second_slot(p, d):
        k = second_base[p] + d - 1
        late = pieces[p][0] // 2
        return second_in[late].at[k], second_sem[late].at[k]

    def partner_term(w, dq, dy, when=None):
        rep = rep_of(at_q(dq), 1 - c, at_y(dy))
        i = w * peers + at_q(dq) * ny + at_y(dy)

        def one():
            @pl.loop(0, n_tiles)
            def _(n):
                partner_out[i, :, n_slice(n)] = term(w, rep, n_slice(n)).astype(BF16)

            pair_copy(i).start()

        guarded(None if when is None else when(rep), one)

    def own_term(w, dq, dy, when=None):
        index = w * peers + at_q(dq) * ny + at_y(dy)
        rep = rep_of(at_q(dq), c, at_y(dy))
        cond = None if when is None else when(rep)

        def one():
            arrived(sums.at[index], pair_recv.at[index])

            @pl.loop(0, n_tiles)
            def _(n):
                ns = n_slice(n)
                sums[index, :, ns] = (term(w, rep, ns) + sums[index, :, ns].astype(F32)).astype(BF16)

        guarded(cond, one)
        for p, (pw, r0, nr, route) in enumerate(pieces):
            if pw == w and (dq if route == 0 else dy):
                dst, sem = first_slot(p, dq, dy)
                where = q_peer(dq) if route == 0 else y_peer(dy)
                sends.start(sums.at[index, pl.ds(r0, nr), :], dst, sem, where, cond)

    grid_order = [(dq, dy) for dq in others_first(nq) for dy in others_first(ny)]

    def terms(w, when=None, order=grid_order):
        for dq, dy in order:
            partner_term(w, dq, dy, when)
        for dq, dy in order:
            own_term(w, dq, dy, when)

    def second_send(p, when=None):
        w, r0, nr, route = pieces[p]
        rs = pl.ds(r0, nr)
        n_first, n_second = (nq, ny) if route == 0 else (ny, nq)
        for d in range(1, n_second):
            index = w * peers + (q * ny + at_y(d) if route == 0 else at_q(d) * ny + y)
            rep = rep_of(q, c, at_y(d)) if route == 0 else rep_of(at_q(d), c, y)
            cond = None if when is None else when(rep)

            def one():
                total = sums[index, rs, :].astype(F32)
                for f in range(1, n_first):
                    ref, sem = first_slot(p, f, d) if route == 0 else first_slot(p, d, f)
                    arrived(ref, sem)
                    total = total + ref[...].astype(F32)
                sums[index, rs, :] = total.astype(BF16)

            guarded(cond, one)
            dst, sem = second_slot(p, d)
            sends.start(sums.at[index, rs, :], dst, sem, y_peer(d) if route == 0 else q_peer(d), cond)

    def second_own(p):
        w, r0, nr, route = pieces[p]
        rs = pl.ds(r0, nr)
        total = sums[w * peers + q * ny + y, rs, :].astype(F32)
        for f in range(1, nq if route == 0 else ny):
            ref, sem = first_slot(p, f, 0) if route == 0 else first_slot(p, 0, f)
            arrived(ref, sem)
            total = total + ref[...].astype(F32)
        outs[w, rs, :] = total

    out_refs = (og_ref, ou_ref, od_ref)
    leaving = []

    def leave(src, dst):
        leaving.append(pltpu.make_async_copy(src, dst, out_sem.at[len(leaving)]))
        leaving[-1].start()

    def second_final(p):
        w, r0, nr, route = pieces[p]
        rs = pl.ds(r0, nr)
        for d in range(1, ny if route == 0 else nq):
            ref, sem = second_slot(p, d)
            arrived(ref, sem)
            outs[w, rs, :] = outs[w, rs, :] + ref[...].astype(F32)
        leave(outs.at[w, rs, :], out_refs[w].at[rs, :])

    near_rep = lambda rep: distance(rep) <= 1
    for step in range(2, n_col - 1):
        terms(2, (lambda s: lambda rep: distance(rep) == s - 1)(step) if step > 2 else near_rep)
        chain(1, step)
    if n_col > 2:
        terms(2, (lambda rep: distance(rep) == n_col - 2) if n_col > 3 else near_rep)
    far_rep = lambda rep: distance(rep) == n_col - 1
    not_far = lambda rep: distance(rep) < n_col - 1
    for p in later:
        near_rest(p)
    for p in later:
        far(p)
    for p in later:
        from_partner(p)

    rest = n_col - 1
    lo = pl.multiple_of(jnp.where(col == n_col - 1, feats, 0), 32)
    last = pl.multiple_of(jnp.where(col == n_col - 1, 0, rest * feats), 32)

    @pl.loop(0, tiles)
    def _(i):
        ms, ns = tile_slices(i)
        ks = pl.ds(lo, rest * feats)
        acc[ms, ns] = lax.dot_general(full[1, ks, ms], weights[2, ks, ns], token_dims, preferred_element_type=F32)

    for p in later:
        second_send(p, not_far)
    chain(1, n_col - 1)

    @pl.loop(0, tiles)
    def _(i):
        ms, ns = tile_slices(i)
        ks = pl.ds(last, feats)
        hidden_grad = acc[ms, ns] + lax.dot_general(
            full[1, ks, ms], weights[2, ks, ns], token_dims, preferred_element_type=F32)
        grads[0, ms, ns] = (hidden_grad * stash[0, ms, ns]).astype(BF16)
        grads[1, ms, ns] = (hidden_grad * stash[1, ms, ns]).astype(BF16)

    terms(2, far_rep)

    rt = tile_of(feats, 288)
    hid_dims = (((1,), (1,)), ((), ()))
    low = col < n_col // 2
    high = jnp.logical_not(low)

    def ig_part(k, h):
        block = jnp.where(low, n_col - 1 - k, k)
        return ig_out.at[block, pl.ds(h * half, half), :], block

    def ig_slot(going_left, d, h):
        k = (going_left * n_col + d) * 2 + h
        return ig_in.at[going_left * (n_col - 1) + d - (1 - going_left), pl.ds(h * half, half), :], ig_sem.at[k]

    def input_part(k):
        block = jnp.where(low, n_col - 1 - k, k)

        @pl.loop(0, feats // rt)
        def _(r):
            rs = pl.ds(pl.multiple_of(block * feats + r * rt, 8), rt)
            part = lax.dot_general(weights[0, rs, :], grads[0], hid_dims, preferred_element_type=F32)
            part = part + lax.dot_general(weights[1, rs, :], grads[1], hid_dims, preferred_element_type=F32)
            ig_out[block, pl.ds(pl.multiple_of(r * rt, 8), rt), :] = part.astype(BF16)

        if k < n_col - 1:
            for h in range(2):
                src = lambda b: ig_out.at[b, pl.ds(h * half, half), :]
                dst, sem = ig_slot(0, n_col - 1 - k, h)
                sends.start(src(n_col - 1 - k), dst, sem, right, col == 0)
                dst, sem = ig_slot(1, k, h)
                sends.start(src(k), dst, sem, left, col == n_col - 1)

    def relay(going_left, k, side=None):
        d = k if going_left else n_col - 1 - k
        inside = (col > d) & (col < n_col - 1) if going_left else (col < d) & (col > 0)
        if side is not None:
            inside = inside & side
        for h in range(2):
            ref, sem = ig_slot(going_left, d, h)
            part = ig_out.at[d, pl.ds(h * half, half), :]

            def one():
                arrived(ref, sem)
                part[...] = (part[...].astype(F32) + ref[...].astype(F32)).astype(BF16)

            guarded(inside, one)
            sends.start(part, ref, sem, left if going_left else right, inside)

    first_off = grid_order[0]
    split = lambda route: [g for g in grid_order if (g[0] if route == 0 else g[1])]
    stay = lambda route: [g for g in grid_order if not (g[0] if route == 0 else g[1])]
    sent = [split(0), split(1)]
    for i in range(max(len(sent[0]), len(sent[1]))):
        for w in range(2):
            if i < len(sent[w]):
                partner_term(w, *sent[w][i])
        for w in range(2):
            if i < len(sent[w]):
                own_term(w, *sent[w][i])
        if i == 0:
            input_part(0)
    for p in later:
        second_send(p, far_rep)
    for k in range(1, n_col - 1):
        input_part(k)
    for w in range(2):
        terms(w, None, stay(w))
    input_part(n_col - 1)
    relay(0, 0, low)
    relay(1, 0, high)
    for p in early:
        second_send(p)
    for p in later:
        second_own(p)
    for p in later:
        second_final(p)
    for k in range(1, n_col - 1):
        relay(0, k, low)
        relay(1, k, high)
    for k in range(n_col - 1):
        relay(1, k, low)
        relay(0, k, high)
    for p in early:
        second_own(p)

    for h in range(2):
        hs = pl.ds(h * half, half)
        from_left, left_sem = ig_slot(0, jnp.maximum(col, 1), h)
        from_right, right_sem = ig_slot(1, jnp.minimum(col, n_col - 2), h)
        guarded(has_left, lambda: arrived(from_left, left_sem))
        guarded(has_right, lambda: arrived(from_right, right_sem))
        own = ig_out[col, hs, :].astype(F32)

        @pl.when(has_left & has_right)
        def _():
            ig_out[col, hs, :] = (own + from_left[...].astype(F32) + from_right[...].astype(F32)).astype(BF16)

        @pl.when(jnp.logical_not(has_left))
        def _():
            ig_out[col, hs, :] = (own + from_right[...].astype(F32)).astype(BF16)

        @pl.when(jnp.logical_not(has_right))
        def _():
            ig_out[col, hs, :] = (own + from_left[...].astype(F32)).astype(BF16)

        leave(ig_out.at[col, hs, :], ig_ref.at[hs, :])
    for p in early:
        second_final(p)
    sends.finish()
    for copy in leaving:
        copy.wait()

    @pl.loop(0, 3 * peers)
    def _(i):
        pair_copy(i).wait_send()


def body(n_dp, n_row, n_col, act_in, cot_out, w_gate, w_up, w_down):
    toks, feats = act_in.shape
    rows, hid = w_gate.shape
    sizes = (n_dp, n_row, n_col, rows, hid, feats, toks)
    nq, ny = n_dp // 2, n_row
    peers, reps, dim = nq * ny, n_dp * n_row, feats * n_col
    pieces = pieces_of(rows)
    firsts, seconds = [0, 0], [0, 0]
    for w, _, _, route in pieces:
        firsts[w // 2] += (nq - 1) * ny if route == 0 else (ny - 1) * nq
        seconds[w // 2] += (ny - 1) if route == 0 else (nq - 1)
    n_pieces = len(pieces)
    n_sends = 8 + 8 * (n_col - 2) + n_pieces * (nq + ny - 1) + n_pieces * (peers - 1) * max(nq, ny)
    n_sends += sum(firsts) * 2 + sum(seconds) * 4 + 4 * (n_col - 1) + 8 * n_col * 3
    late_rows = min(nr for w, _, nr, _ in pieces if w == 2)
    any_spec = pl.BlockSpec(memory_space=pl.ANY)
    dma = lambda n: pltpu.SemaphoreType.DMA((max(n, 1),))
    landing = lambda n: [pltpu.VMEM((max(n[0], 1), rows, hid), BF16), pltpu.VMEM((max(n[1], 1), late_rows, hid), BF16)]
    wgrad = jax.ShapeDtypeStruct((rows, hid), F32)
    ig_t, gate_grad, up_grad, down_t = pl.pallas_call(
        functools.partial(kernel, sizes),
        out_shape=[jax.ShapeDtypeStruct((feats, toks), BF16), wgrad, wgrad, wgrad],
        in_specs=[any_spec] * 5,
        out_specs=[any_spec] * 4,
        scratch_shapes=[
            pltpu.VMEM((2, dim, toks), BF16),
            pltpu.VMEM((3, dim, hid), BF16),
            pltpu.VMEM((3, toks, hid), BF16),
            pltpu.VMEM((2, toks, hid), F32),
            pltpu.VMEM((toks, hid), F32),
            pltpu.VMEM((3 * peers, rows, hid), BF16),
            pltpu.VMEM((3 * peers, rows, hid), BF16),
            landing(firsts),
            landing(seconds),
            pltpu.VMEM((n_col, feats, toks), BF16),
            pltpu.VMEM((2 * (n_col - 1), feats, toks), BF16),
            pltpu.VMEM((3, rows, hid), F32),
            dma(5), dma(n_sends), dma(n_pieces * reps), dma(4 * n_col), dma(3 * peers), dma(3 * peers),
            [dma(n) for n in firsts], [dma(n) for n in seconds], dma(4 * n_col), dma(n_pieces + 2),
        ],
        compiler_params=pltpu.CompilerParams(
            collective_id=0, has_side_effects=True, vmem_limit_bytes=67043328
        ),
    )(act_in.T, cot_out.T, w_gate, w_up, w_down.T)
    norm_scale = 1.0 / math.sqrt(toks * n_dp * n_row)
    return (ig_t.T, gate_grad * norm_scale, up_grad * norm_scale, (down_t * norm_scale).T)


def solution(mesh):
    grid = P(("dp", "row"), "col")
    flipped = P("col", ("dp", "row"))
    return jax.shard_map(
        functools.partial(body, mesh.shape["dp"], mesh.shape["row"], mesh.shape["col"]),
        mesh=mesh,
        in_specs=(grid, grid, grid, grid, flipped),
        out_specs=(grid, grid, grid, flipped),
        check_vma=False,
    )
```

```python
import functools
import math

import jax
import jax.numpy as jnp
from jax import lax
from jax.experimental import pallas as pl
from jax.experimental.pallas import tpu as pltpu
from jax.sharding import PartitionSpec as P

gelu_cubic = 0.044715
gelu_scale = 0.7978845608028654
MESH = pl.DeviceIdType.MESH
F32 = jnp.float32
BF16 = jnp.bfloat16


def gelu_parts(values):
    inner_arg = gelu_scale * (values + gelu_cubic * values * values * values)
    tanh_val = jnp.tanh(inner_arg)
    output = 0.5 * values * (1.0 + tanh_val)
    slope_val = 0.5 * (1.0 + tanh_val) + 0.5 * values * (1.0 - tanh_val * tanh_val) * gelu_scale * (
        1.0 + 3.0 * gelu_cubic * values * values
    )
    return (output, slope_val)


def tile_of(size, best):
    return best if size % best == 0 else size


def pieces_of(rows):
    if rows % 32 == 0:
        return [(0, 0, rows, 0), (1, 0, rows, 1), (2, 0, rows // 2, 0), (2, rows // 2, rows // 2, 1)]
    return [(0, 0, rows, 0), (1, 0, rows, 1), (2, 0, rows, 0)]


def others_first(n):
    return list(range(1, n)) + [0]


class Sends:
    def __init__(self, sems):
        self.sems, self.used, self.pending = sems, 0, []

    def start(self, src, dst, recv_sem, where, cond=None):
        copy = pltpu.make_async_remote_copy(
            src_ref=src,
            dst_ref=dst,
            send_sem=self.sems.at[self.used],
            recv_sem=recv_sem,
            device_id=where,
            device_id_type=MESH,
        )
        self.used += 1
        self.pending.append((cond, copy))
        guarded(cond, copy.start)

    def finish(self):
        for cond, copy in self.pending:
            guarded(cond, copy.wait_send)


def guarded(cond, action):
    if cond is None:
        action()
    else:
        pl.when(cond)(action)


def arrived(ref, sem):
    pltpu.make_async_copy(ref, ref, sem).wait()


def kernel(sizes, act_ref, cot_ref, wg_ref, wu_ref, wd_ref, ig_ref, og_ref, ou_ref, od_ref,
           full, weights, grads, stash, acc, partner_out, sums, first_in, second_in, ig_out, ig_in,
           own_sem, send_sem, w_sem, x_sem, pair_send, pair_recv, first_sem, second_sem, ig_sem, slice_sem):
    n_dp, n_row, n_col, rows, hid, feats, toks = sizes
    nq, ny = n_dp // 2, n_row
    peers = nq * ny
    pieces = pieces_of(rows)
    dp, y, col = lax.axis_index("dp"), lax.axis_index("row"), lax.axis_index("col")
    q, c = dp // 2, dp % 2
    rep_of = lambda q1, c1, y1: (q1 * 2 + c1) * ny + y1
    at_q = lambda dq: lax.rem(q + dq, nq)
    at_y = lambda dy: lax.rem(y + dy, ny)
    back_q = lambda dq: lax.rem(q + nq - dq, nq)
    back_y = lambda dy: lax.rem(y + ny - dy, ny)
    me = rep_of(q, c, y)
    partner = {"dp": q * 2 + 1 - c}
    q_peer = lambda dq: {"dp": at_q(dq) * 2 + c}
    y_peer = lambda dy: {"row": at_y(dy)}
    xs, ys = [q_peer(i) for i in range(1, nq)], [y_peer(i) for i in range(1, ny)]

    barrier = pltpu.get_barrier_semaphore()
    friends = [partner] + xs + ys
    for friend in friends:
        pl.semaphore_signal(barrier, inc=1, device_id=friend, device_id_type=MESH)
    has_right, has_left = col < n_col - 1, col > 0
    right = {"col": jnp.minimum(col + 1, n_col - 1)}
    left = {"col": jnp.maximum(col - 1, 0)}
    for there, friend in ((has_right, right), (has_left, left)):
        @pl.when(there)
        def _():
            pl.semaphore_signal(barrier, inc=1, device_id=friend, device_id_type=MESH)
    pl.semaphore_wait(barrier, len(friends) + has_right.astype(jnp.int32) + has_left.astype(jnp.int32))

    sends = Sends(send_sem)
    mine = (wg_ref, wu_ref, wd_ref)
    streams = (act_ref, cot_ref)

    def rows_at(rep, r0, nr):
        return pl.ds(pl.multiple_of(rep * rows + r0, 8), nr)

    def slot(p, rep):
        w, r0, nr, _ = pieces[p]
        return weights.at[w, rows_at(rep, r0, nr), :]

    half = feats // 2

    def feat_slot(s, h, block):
        return full.at[s, pl.ds(pl.multiple_of(block * feats + h * half, 8), half), :]

    def feat_sem(s, h, block):
        return x_sem.at[(s * 2 + h) * n_col + block]

    at_end = (col == 0) | (col == n_col - 1)
    middle = jnp.logical_not(at_end)
    low = col < n_col // 2
    high = jnp.logical_not(low)
    staggered = n_col == 4 and nq == 2 and rows == half

    def own_features(s, to_right, to_left, halves=range(2)):
        for h in halves:
            src = streams[s].at[pl.ds(h * half, half), :]
            sends.start(src, feat_slot(s, h, col), feat_sem(s, h, col), right, to_right)
            sends.start(src, feat_slot(s, h, col), feat_sem(s, h, col), left, to_left)

    def own_piece(p, wheres):
        w, r0, nr, _ = pieces[p]
        for where in wheres:
            sends.start(mine[w].at[pl.ds(r0, nr), :], slot(p, me), w_sem.at[p * peers * 2 + me], where)

    early = [p for p in range(len(pieces)) if pieces[p][0] < 2]
    later = [p for p in range(len(pieces)) if pieces[p][0] == 2]
    own_features(0, has_right, has_left)
    own_features(1, has_right & at_end, has_left & at_end)
    for p in early:
        own_piece(p, xs)
    for p in reversed(early):
        own_piece(p, ys)
    for p in early:
        own_piece(p, [partner])
    locals_ = []
    for i, (src, dst) in enumerate(
        [(streams[s], full.at[s, pl.ds(pl.multiple_of(col * feats, 8), feats), :]) for s in range(2)]
        + [(mine[w], weights.at[w, rows_at(me, 0, rows), :]) for w in range(3)]
    ):
        locals_.append(pltpu.make_async_copy(src, dst, own_sem.at[i]))
        locals_[-1].start()

    def chain(s, step, when_left, when_right):
        from_left, from_right = (col >= step) & when_left, (col + step < n_col) & when_right
        lb, rb = jnp.maximum(col - step, 0), jnp.minimum(col + step, n_col - 1)
        for h in range(2):
            l_slot, l_sem = feat_slot(s, h, lb), feat_sem(s, h, lb)
            r_slot, r_sem = feat_slot(s, h, rb), feat_sem(s, h, rb)
            guarded(from_left, lambda: arrived(l_slot, l_sem))
            if step < n_col - 1:
                sends.start(l_slot, l_slot, l_sem, right, from_left & has_right)
            guarded(from_right, lambda: arrived(r_slot, r_sem))
            if step < n_col - 1:
                sends.start(r_slot, r_slot, r_sem, left, from_right & has_left)

    late_end = at_end if staggered else col < 0
    late_mid = middle if staggered else col < 0

    def end_wait(d, halves, when):
        block = jnp.where(low, d, n_col - 1 - d)
        for h in halves:
            guarded(at_end & when, lambda: arrived(feat_slot(1, h, block), feat_sem(1, h, block)))

    def take(p, rep, forward):
        sem = w_sem.at[p * peers * 2 + rep]
        arrived(slot(p, rep), sem)
        for where in forward + [partner]:
            sends.start(slot(p, rep), slot(p, rep), sem, where)

    def near_first(p):
        if pieces[p][3] == 0:
            for dq in range(1, nq):
                take(p, rep_of(back_q(dq), c, y), ys)
        else:
            for dy in range(1, ny):
                take(p, rep_of(q, c, back_y(dy)), xs)

    def near_rest(p):
        if pieces[p][3] == 0:
            for dy in range(1, ny):
                take(p, rep_of(q, c, back_y(dy)), [])
        else:
            for dq in range(1, nq):
                take(p, rep_of(back_q(dq), c, y), [])

    def far(p):
        for dq in range(1, nq):
            for dy in range(1, ny):
                take(p, rep_of(back_q(dq), c, back_y(dy)), [])

    def from_partner(p):
        for dq in range(nq):
            for dy in range(ny):
                rep = rep_of(at_q(dq), 1 - c, at_y(dy))
                arrived(slot(p, rep), w_sem.at[p * peers * 2 + rep])

    always = col >= 0
    chain(0, 1, always, always)
    if n_col == 4:
        own_features(1, middle & low, middle & high)
    for p in early:
        near_first(p)
    for p in later:
        own_piece(p, xs)
    for p in reversed(later):
        own_piece(p, ys)
    for p in later:
        own_piece(p, [partner])
    for step in range(2, n_col - 1):
        chain(0, step, always, always)
    prompt = jnp.logical_not(late_mid)
    if n_col == 4:
        own_features(1, middle & high, middle & low, [0])
        own_features(1, middle & high & prompt, middle & low & prompt, [1])
        chain(1, 1, middle & low, middle & high)
    else:
        own_features(1, middle, middle)
    for p in early:
        near_rest(p)
    if n_col > 2:
        chain(0, n_col - 1, always, always)
    if n_col == 4:
        chain(1, 1, middle & high, middle & low)
    else:
        chain(1, 1, middle, middle)
    for p in early:
        far(p)
    for p in early:
        from_partner(p)
    for copy in locals_:
        copy.wait()

    mt, nt = tile_of(toks, 256), tile_of(hid, 384)
    m_tiles, n_tiles = toks // mt, hid // nt
    token_dims = (((0,), (0,)), ((), ()))

    def tile_slices(i):
        m, n = i // n_tiles, i % n_tiles
        return pl.ds(pl.multiple_of(m * mt, mt), mt), pl.ds(pl.multiple_of(n * nt, nt), nt)

    def project(first, last):
        @pl.loop(first, last)
        def _(i):
            ms, ns = tile_slices(i)
            x = full[0, :, ms]
            gate_pre = lax.dot_general(x, weights[0, :, ns], token_dims, preferred_element_type=F32)
            up_pre = lax.dot_general(x, weights[1, :, ns], token_dims, preferred_element_type=F32)
            act_val, slope_val = gelu_parts(gate_pre)
            grads[2, ms, ns] = (act_val * up_pre).astype(BF16)
            stash[0, ms, ns] = up_pre * slope_val
            stash[1, ms, ns] = act_val

    tiles = m_tiles * n_tiles
    project(0, tiles // 2)
    for p in later:
        near_first(p)
    for step in range(2, n_col - 1):
        chain(1, step, middle, middle)
    if staggered:
        own_features(1, middle & high & late_mid, middle & low & late_mid, [1])
    project(tiles // 2, tiles)

    def term(w, rep):
        return jnp.dot(full[w // 2, rows_at(rep, 0, rows), :], grads[w], preferred_element_type=F32)

    def pair_copy(i):
        return pltpu.make_async_remote_copy(
            src_ref=partner_out.at[lax.rem(i, 2 * peers)],
            dst_ref=sums.at[i],
            send_sem=pair_send.at[i],
            recv_sem=pair_recv.at[i],
            device_id=partner,
            device_id_type=MESH,
        )

    last_stage = max(n_col - 2, 0)

    def stage_of(rep, late):
        block = (rep * rows) // feats
        dist = jnp.abs(block - col)
        plain = jnp.maximum(dist - 1, 0)
        if not staggered:
            return plain
        second_half = lax.rem(rep, feats // rows) == 1
        shifted = jnp.where(dist == 1, jnp.where(second_half, 2, 0), jnp.maximum(dist - 2, 0))
        return jnp.where(late, shifted, plain)

    def own_stage(rep):
        return stage_of(rep, late_end)

    def sum_stage(rep, route):
        return own_stage(rep)

    first_base, count = [], [0, 0]
    for w, _, _, route in pieces:
        first_base.append(count[w // 2])
        count[w // 2] += (nq - 1) * ny if route == 0 else (ny - 1) * nq
    second_base, count = [], [0, 0]
    for w, _, _, route in pieces:
        second_base.append(count[w // 2])
        count[w // 2] += (ny - 1) if route == 0 else (nq - 1)

    def first_slot(p, dq, dy):
        k = first_base[p] + ((dq - 1) * ny + dy if pieces[p][3] == 0 else (dy - 1) * nq + dq)
        late = pieces[p][0] // 2
        return first_in[late].at[k], first_sem[late].at[k]

    def second_slot(p, d):
        k = second_base[p] + d - 1
        late = pieces[p][0] // 2
        return second_in[late].at[k], second_sem[late].at[k]

    def partner_term(w, dq, dy, when=None):
        rep = rep_of(at_q(dq), 1 - c, at_y(dy))
        i = w * peers + at_q(dq) * ny + at_y(dy)

        def one():
            if w == 0:
                pair_copy(2 * peers + i).wait_send()
            partner_out[lax.rem(i, 2 * peers)] = term(w, rep).astype(BF16)
            pair_copy(i).start()

        guarded(None if when is None else when(rep), one)

    def slice_copy(p, dq, dy):
        w, r0, nr, route = pieces[p]
        index = w * peers + at_q(dq) * ny + at_y(dy)
        dst, sem = first_slot(p, dq, dy)
        return pltpu.make_async_remote_copy(
            src_ref=sums.at[index, pl.ds(r0, nr), :],
            dst_ref=dst,
            send_sem=slice_sem.at[p * peers + dq * ny + dy],
            recv_sem=sem,
            device_id=q_peer(dq) if route == 0 else y_peer(dy),
            device_id_type=MESH,
        )

    def own_term(w, dq, dy, when=None):
        index = w * peers + at_q(dq) * ny + at_y(dy)
        rep = rep_of(at_q(dq), c, at_y(dy))

        def one():
            arrived(sums.at[index], pair_recv.at[index])
            sums[index] = (term(w, rep) + sums[index].astype(F32)).astype(BF16)
            for p, (pw, _, _, route) in enumerate(pieces):
                if pw == w:
                    away = dq if route == 0 else dy
                    if not isinstance(away, int):
                        pl.when(away > 0)(slice_copy(p, dq, dy).start)
                    elif away:
                        slice_copy(p, dq, dy).start()

        guarded(None if when is None else when(rep), one)

    grid_order = [(dq, dy) for dq in others_first(nq) for dy in others_first(ny)]

    def place(i):
        return lax.rem(1 + i // ny, nq), lax.rem(1 + i % ny, ny)

    def partner_terms(w, when=None):
        @pl.loop(0, peers)
        def _(i):
            partner_term(w, *place(i), when)

    def own_terms(w, when=None):
        @pl.loop(0, peers)
        def _(i):
            own_term(w, *place(i), when)

    def second_send(p, when=None):
        w, r0, nr, route = pieces[p]
        rs = pl.ds(r0, nr)
        n_first, n_second = (nq, ny) if route == 0 else (ny, nq)
        for d in range(1, n_second):
            index = w * peers + (q * ny + at_y(d) if route == 0 else at_q(d) * ny + y)
            rep = rep_of(q, c, at_y(d)) if route == 0 else rep_of(at_q(d), c, y)
            cond = None if when is None else when(sum_stage(rep, route))

            def one():
                total = sums[index, rs, :].astype(F32)
                for f in range(1, n_first):
                    ref, sem = first_slot(p, f, d) if route == 0 else first_slot(p, d, f)
                    arrived(ref, sem)
                    total = total + ref[...].astype(F32)
                sums[index, rs, :] = total.astype(BF16)

            guarded(cond, one)
            dst, sem = second_slot(p, d)
            sends.start(sums.at[index, rs, :], dst, sem, y_peer(d) if route == 0 else q_peer(d), cond)

    outs = (og_ref, ou_ref, od_ref)

    def second_own(p):
        w, r0, nr, route = pieces[p]
        rs = pl.ds(r0, nr)
        total = sums[w * peers + q * ny + y, rs, :].astype(F32)
        for f in range(1, nq if route == 0 else ny):
            ref, sem = first_slot(p, f, 0) if route == 0 else first_slot(p, 0, f)
            arrived(ref, sem)
            total = total + ref[...].astype(F32)
        outs[w][rs, :] = total

    def second_final(p):
        w, r0, nr, route = pieces[p]
        rs = pl.ds(r0, nr)
        for d in range(1, ny if route == 0 else nq):
            ref, sem = second_slot(p, d)
            arrived(ref, sem)
            outs[w][rs, :] = outs[w][rs, :] + ref[...].astype(F32)

    stage_is = lambda k: lambda rep: own_stage(rep) == k
    on_time = jnp.logical_not(late_end)
    for k in range(last_stage):
        if k == 0:
            end_wait(1, range(2), on_time)
            if staggered:
                end_wait(1, [0], late_end)
                end_wait(2, range(2), late_end)
        else:
            end_wait(k + 1, range(2), on_time)
            if staggered:
                end_wait(k + 2, range(2), late_end)
        partner_terms(2, stage_is(k))
        own_terms(2, stage_is(k))
        if k == 0:
            for p in later:
                near_rest(p)
            for p in later:
                far(p)
    for p in later:
        from_partner(p)

    inner = max(n_col - 2, 0) * feats
    single = pl.multiple_of(jnp.where(low, 0, n_col - 1) * feats, 32)
    pair = pl.multiple_of(jnp.where(late_end, jnp.where(low, 2, 0), 1) * feats, 32)
    last = pl.multiple_of(
        jnp.where(late_end, jnp.where(low, 1, n_col - 2), jnp.where(low, n_col - 1, 0)) * feats, 32)

    @pl.loop(0, m_tiles)
    def _(m):
        ms = pl.ds(pl.multiple_of(m * mt, mt), mt)
        ks = pl.ds(single, feats)
        part = lax.dot_general(full[1, ks, ms], weights[2, ks, :], token_dims, preferred_element_type=F32)
        if inner:
            ks = pl.ds(pair, inner)
            part = part + lax.dot_general(full[1, ks, ms], weights[2, ks, :], token_dims, preferred_element_type=F32)
        acc[ms, :] = part

    for p in later:
        second_send(p, lambda k: k < last_stage - 1)
    end_wait(n_col - 1, range(2), on_time)
    if staggered:
        end_wait(1, [1], late_end)
    partner_terms(2, stage_is(last_stage))

    @pl.loop(0, m_tiles)
    def _(m):
        ms = pl.ds(pl.multiple_of(m * mt, mt), mt)
        ks = pl.ds(last, feats)
        acc[ms, :] = acc[ms, :] + lax.dot_general(
            full[1, ks, ms], weights[2, ks, :], token_dims, preferred_element_type=F32)

    et = tile_of(toks, 32)

    @pl.loop(0, toks // et)
    def _(m):
        ms = pl.ds(pl.multiple_of(m * et, et), et)
        hidden_grad = acc[ms, :]
        grads[0, ms, :] = (hidden_grad * stash[0, ms, :]).astype(BF16)
        grads[1, ms, :] = (hidden_grad * stash[1, ms, :]).astype(BF16)

    rt = tile_of(feats, 288)
    hid_dims = (((1,), (1,)), ((), ()))

    def ig_slot(going_left, d, h):
        k = (going_left * n_col + d) * 2 + h
        return ig_in.at[going_left * (n_col - 1) + d - (1 - going_left), pl.ds(h * half, half), :], ig_sem.at[k]

    def input_part(k):
        block = jnp.where(low, n_col - 1 - k, k)

        @pl.loop(0, feats // rt)
        def _(r):
            rs = pl.ds(pl.multiple_of(block * feats + r * rt, 8), rt)
            part = lax.dot_general(weights[0, rs, :], grads[0], hid_dims, preferred_element_type=F32)
            part = part + lax.dot_general(weights[1, rs, :], grads[1], hid_dims, preferred_element_type=F32)
            ig_out[block, pl.ds(pl.multiple_of(r * rt, 8), rt), :] = part.astype(BF16)

        if k < n_col - 1:
            for h in range(2):
                src = lambda b: ig_out.at[b, pl.ds(h * half, half), :]
                dst, sem = ig_slot(0, n_col - 1 - k, h)
                sends.start(src(n_col - 1 - k), dst, sem, right, col == 0)
                dst, sem = ig_slot(1, k, h)
                sends.start(src(k), dst, sem, left, col == n_col - 1)

    def relay(going_left, k, side=None):
        d = k if going_left else n_col - 1 - k
        inside = (col > d) & (col < n_col - 1) if going_left else (col < d) & (col > 0)
        if side is not None:
            inside = inside & side
        for h in range(2):
            ref, sem = ig_slot(going_left, d, h)
            part = ig_out.at[d, pl.ds(h * half, half), :]

            def one():
                arrived(ref, sem)
                part[...] = (part[...].astype(F32) + ref[...].astype(F32)).astype(BF16)

            guarded(inside, one)
            sends.start(part, ref, sem, left if going_left else right, inside)

    sent = [[g for g in grid_order if g[0]], [g for g in grid_order if g[1]]]
    for i in range(max(len(sent[0]), len(sent[1]))):
        both = [(w, sent[w][i]) for w in range(2) if i < len(sent[w])]
        for w, place_i in both:
            partner_term(w, *place_i)
        if i == 0:
            own_terms(2, stage_is(last_stage))
        for w, place_i in both:
            own_term(w, *place_i)
        if i == 0:
            for p in later:
                second_send(p, lambda k: k == last_stage - 1)
            input_part(0)
    for p in later:
        second_send(p, lambda k: k == last_stage)
    for k in range(1, n_col - 1):
        input_part(k)
    for w in range(2):
        @pl.loop(0, peers // (nq if w == 0 else ny))
        def _(i):
            j = lax.rem(i + 1, ny if w == 0 else nq)
            partner_term(w, *((0, j) if w == 0 else (j, 0)))

        @pl.loop(0, peers // (nq if w == 0 else ny))
        def _(i):
            j = lax.rem(i + 1, ny if w == 0 else nq)
            own_term(w, *((0, j) if w == 0 else (j, 0)))

    input_part(n_col - 1)
    relay(0, 0, low)
    relay(1, 0, high)
    for p in early:
        second_send(p)
    for k in range(1, n_col - 1):
        relay(0, k, low)
        relay(1, k, high)
    for k in range(n_col - 1):
        relay(1, k, low)
        relay(0, k, high)
    for p in early:
        second_own(p)
    for p in later:
        second_own(p)
    for p in later:
        second_final(p)

    for h in range(2):
        hs = pl.ds(h * half, half)
        from_left, left_sem = ig_slot(0, jnp.maximum(col, 1), h)
        from_right, right_sem = ig_slot(1, jnp.minimum(col, n_col - 2), h)
        guarded(has_left, lambda: arrived(from_left, left_sem))
        guarded(has_right, lambda: arrived(from_right, right_sem))
        own = ig_out[col, hs, :].astype(F32)

        @pl.when(has_left & has_right)
        def _():
            ig_ref[hs, :] = (own + from_left[...].astype(F32) + from_right[...].astype(F32)).astype(BF16)

        @pl.when(jnp.logical_not(has_left))
        def _():
            ig_ref[hs, :] = (own + from_right[...].astype(F32)).astype(BF16)

        @pl.when(jnp.logical_not(has_right))
        def _():
            ig_ref[hs, :] = (own + from_left[...].astype(F32)).astype(BF16)

    for p in early:
        second_final(p)
    sends.finish()

    @pl.loop(0, 2 * peers)
    def _(i):
        pair_copy(i).wait_send()

    for p, (_, _, _, route) in enumerate(pieces):
        @pl.loop(0, peers)
        def _(i):
            dq, dy = i // ny, i % ny
            pl.when((dq if route == 0 else dy) > 0)(slice_copy(p, dq, dy).wait_send)


def body(n_dp, n_row, n_col, act_in, cot_out, w_gate, w_up, w_down):
    toks, feats = act_in.shape
    rows, hid = w_gate.shape
    sizes = (n_dp, n_row, n_col, rows, hid, feats, toks)
    nq, ny = n_dp // 2, n_row
    peers, reps, dim = nq * ny, n_dp * n_row, feats * n_col
    pieces = pieces_of(rows)
    firsts, seconds = [0, 0], [0, 0]
    for w, _, _, route in pieces:
        firsts[w // 2] += (nq - 1) * ny if route == 0 else (ny - 1) * nq
        seconds[w // 2] += (ny - 1) if route == 0 else (nq - 1)
    n_pieces = len(pieces)
    n_sends = 24 + 8 * n_col + n_pieces * (nq + ny - 1) + n_pieces * (peers - 1) * max(nq, ny)
    n_sends += sum(firsts) * 2 + sum(seconds) * 4 + 4 * (n_col - 1) + 8 * n_col * 3
    late_rows = min(nr for w, _, nr, _ in pieces if w == 2)
    any_spec = pl.BlockSpec(memory_space=pl.ANY)
    dma = lambda n: pltpu.SemaphoreType.DMA((max(n, 1),))
    landing = lambda n: [pltpu.VMEM((max(n[0], 1), rows, hid), BF16), pltpu.VMEM((max(n[1], 1), late_rows, hid), BF16)]
    wgrad = pltpu.VMEM((rows, hid), F32)
    ig_t, gate_grad, up_grad, down_t = pl.pallas_call(
        functools.partial(kernel, sizes),
        out_shape=[pltpu.VMEM((feats, toks), BF16), wgrad, wgrad, wgrad],
        in_specs=[any_spec] * 5,
        out_specs=[pl.BlockSpec(memory_space=pltpu.VMEM)] * 4,
        scratch_shapes=[
            pltpu.VMEM((2, dim, toks), BF16),
            pltpu.VMEM((3, dim, hid), BF16),
            pltpu.VMEM((3, toks, hid), BF16),
            pltpu.VMEM((2, toks, hid), F32),
            pltpu.VMEM((toks, hid), F32),
            pltpu.VMEM((2 * peers, rows, hid), BF16),
            pltpu.VMEM((3 * peers, rows, hid), BF16),
            landing(firsts),
            landing(seconds),
            pltpu.VMEM((n_col, feats, toks), BF16),
            pltpu.VMEM((2 * (n_col - 1), feats, toks), BF16),
            dma(5), dma(n_sends), dma(n_pieces * reps), dma(4 * n_col), dma(3 * peers), dma(3 * peers),
            [dma(n) for n in firsts], [dma(n) for n in seconds], dma(4 * n_col),
            dma(n_pieces * peers),
        ],
        compiler_params=pltpu.CompilerParams(
            collective_id=0, has_side_effects=True, vmem_limit_bytes=60600000
        ),
    )(act_in.T, cot_out.T, w_gate, w_up, w_down.T)
    norm_scale = 1.0 / math.sqrt(toks * n_dp * n_row)
    return (ig_t.T, gate_grad * norm_scale, up_grad * norm_scale, (down_t * norm_scale).T)


def solution(mesh):
    grid = P(("dp", "row"), "col")
    flipped = P("col", ("dp", "row"))
    return jax.shard_map(
        functools.partial(body, mesh.shape["dp"], mesh.shape["row"], mesh.shape["col"]),
        mesh=mesh,
        in_specs=(grid, grid, grid, grid, flipped),
        out_specs=(grid, grid, grid, flipped),
        check_vma=False,
    )
```

```python
import functools
import math

import jax
import jax.numpy as jnp
from jax import lax
from jax.experimental import pallas as pl
from jax.experimental.pallas import tpu as pltpu
from jax.sharding import PartitionSpec as P

gelu_cubic = 0.044715
gelu_scale = 0.7978845608028654
MESH = pl.DeviceIdType.MESH
F32 = jnp.float32
BF16 = jnp.bfloat16


def gelu_parts(values):
    inner_arg = gelu_scale * (values + gelu_cubic * values * values * values)
    tanh_val = jnp.tanh(inner_arg)
    output = 0.5 * values * (1.0 + tanh_val)
    slope_val = 0.5 * (1.0 + tanh_val) + 0.5 * values * (1.0 - tanh_val * tanh_val) * gelu_scale * (
        1.0 + 3.0 * gelu_cubic * values * values
    )
    return (output, slope_val)


def tile_of(size, best):
    return best if size % best == 0 else size


def pieces_of(rows):
    if rows % 32 == 0:
        return [(0, 0, rows, 0), (1, 0, rows, 1), (2, 0, rows // 2, 0), (2, rows // 2, rows // 2, 1)]
    return [(0, 0, rows, 0), (1, 0, rows, 1), (2, 0, rows, 0)]


def others_first(n):
    return list(range(1, n)) + [0]


class Sends:
    def __init__(self, sems):
        self.sems, self.spots, self.pending = sems, {}, []

    def start(self, src, dst, recv_sem, where, cond=None, spot=None):
        spot = self.spots.setdefault(len(self.pending) if spot is None else spot, len(self.spots))
        copy = pltpu.make_async_remote_copy(
            src_ref=src,
            dst_ref=dst,
            send_sem=self.sems.at[spot],
            recv_sem=recv_sem,
            device_id=where,
            device_id_type=MESH,
        )
        self.pending.append((cond, copy))
        guarded(cond, copy.start)

    def finish(self):
        for cond, copy in self.pending:
            guarded(cond, copy.wait_send)


def guarded(cond, action):
    if cond is None:
        action()
    else:
        pl.when(cond)(action)


def arrived(ref, sem):
    pltpu.make_async_copy(ref, ref, sem).wait()


def kernel(sizes, act_ref, cot_ref, wg_ref, wu_ref, wd_ref, ig_ref, og_ref, ou_ref, od_ref,
           full, weights, grads, stash, acc, partner_out, sums, first_in, second_in, ig_out, ig_in,
           own_sem, send_sem, w_sem, x_sem, pair_send, pair_recv, first_sem, second_sem, ig_sem, slice_sem):
    n_dp, n_row, n_col, rows, hid, feats, toks = sizes
    nq, ny = n_dp // 2, n_row
    peers = nq * ny
    pieces = pieces_of(rows)
    dp, y, col = lax.axis_index("dp"), lax.axis_index("row"), lax.axis_index("col")
    q, c = dp // 2, dp % 2
    rep_of = lambda q1, c1, y1: (q1 * 2 + c1) * ny + y1
    at_q = lambda dq: lax.rem(q + dq, nq)
    at_y = lambda dy: lax.rem(y + dy, ny)
    back_q = lambda dq: lax.rem(q + nq - dq, nq)
    back_y = lambda dy: lax.rem(y + ny - dy, ny)
    me = rep_of(q, c, y)
    partner = {"dp": q * 2 + 1 - c}
    q_peer = lambda dq: {"dp": at_q(dq) * 2 + c}
    y_peer = lambda dy: {"row": at_y(dy)}
    xs, ys = [q_peer(i) for i in range(1, nq)], [y_peer(i) for i in range(1, ny)]

    barrier = pltpu.get_barrier_semaphore()
    friends = [partner] + xs + ys
    for friend in friends:
        pl.semaphore_signal(barrier, inc=1, device_id=friend, device_id_type=MESH)
    has_right, has_left = col < n_col - 1, col > 0
    right = {"col": jnp.minimum(col + 1, n_col - 1)}
    left = {"col": jnp.maximum(col - 1, 0)}
    for there, friend in ((has_right, right), (has_left, left)):
        @pl.when(there)
        def _():
            pl.semaphore_signal(barrier, inc=1, device_id=friend, device_id_type=MESH)
    pl.semaphore_wait(barrier, len(friends) + has_right.astype(jnp.int32) + has_left.astype(jnp.int32))

    sends = Sends(send_sem)
    mine = (wg_ref, wu_ref, wd_ref)
    streams = (act_ref, cot_ref)

    def rows_at(rep, r0, nr):
        return pl.ds(pl.multiple_of(rep * rows + r0, 8), nr)

    def slot(p, rep):
        w, r0, nr, _ = pieces[p]
        return weights.at[w, rows_at(rep, r0, nr), :]

    half = feats // 2

    def feat_slot(s, h, block):
        return full.at[s, pl.ds(pl.multiple_of(block * feats + h * half, 8), half), :]

    def feat_sem(s, h, block):
        return x_sem.at[(s * 2 + h) * n_col + block]

    at_end = (col == 0) | (col == n_col - 1)
    middle = jnp.logical_not(at_end)
    low = col < n_col // 2
    high = jnp.logical_not(low)
    staggered = n_col == 4 and nq == 2 and rows == half

    def own_features(s, to_right, to_left, halves=range(2)):
        for h in halves:
            src = streams[s].at[pl.ds(h * half, half), :]
            sends.start(src, feat_slot(s, h, col), feat_sem(s, h, col), right, to_right, ("own", s, h, 0))
            sends.start(src, feat_slot(s, h, col), feat_sem(s, h, col), left, to_left, ("own", s, h, 1))

    def own_piece(p, wheres):
        w, r0, nr, _ = pieces[p]
        for where in wheres:
            sends.start(mine[w].at[pl.ds(r0, nr), :], slot(p, me), w_sem.at[p * peers * 2 + me], where)

    early = [p for p in range(len(pieces)) if pieces[p][0] < 2]
    later = [p for p in range(len(pieces)) if pieces[p][0] == 2]
    own_features(0, has_right, has_left)
    own_features(1, has_right & at_end, has_left & at_end)
    for p in early:
        own_piece(p, xs)
    for p in reversed(early):
        own_piece(p, ys)
    for p in early:
        own_piece(p, [partner])
    locals_ = []
    for i, (src, dst) in enumerate(
        [(streams[s], full.at[s, pl.ds(pl.multiple_of(col * feats, 8), feats), :]) for s in range(2)]
        + [(mine[w], weights.at[w, rows_at(me, 0, rows), :]) for w in range(3)]
    ):
        locals_.append(pltpu.make_async_copy(src, dst, own_sem.at[i]))
        locals_[-1].start()

    def chain(s, step, when_left, when_right):
        from_left, from_right = (col >= step) & when_left, (col + step < n_col) & when_right
        lb, rb = jnp.maximum(col - step, 0), jnp.minimum(col + step, n_col - 1)
        for h in range(2):
            l_slot, l_sem = feat_slot(s, h, lb), feat_sem(s, h, lb)
            r_slot, r_sem = feat_slot(s, h, rb), feat_sem(s, h, rb)
            guarded(from_left, lambda: arrived(l_slot, l_sem))
            if step < n_col - 1:
                sends.start(l_slot, l_slot, l_sem, right, from_left & has_right, ("on", s, step, h, 0))
            guarded(from_right, lambda: arrived(r_slot, r_sem))
            if step < n_col - 1:
                sends.start(r_slot, r_slot, r_sem, left, from_right & has_left, ("on", s, step, h, 1))

    late_end = at_end if staggered else col < 0
    late_mid = middle if staggered else col < 0

    def end_wait(d, halves, when):
        block = jnp.where(low, d, n_col - 1 - d)
        for h in halves:
            guarded(at_end & when, lambda: arrived(feat_slot(1, h, block), feat_sem(1, h, block)))

    def take(p, rep, forward):
        sem = w_sem.at[p * peers * 2 + rep]
        arrived(slot(p, rep), sem)
        for where in forward + [partner]:
            sends.start(slot(p, rep), slot(p, rep), sem, where)

    def near_first(p):
        if pieces[p][3] == 0:
            for dq in range(1, nq):
                take(p, rep_of(back_q(dq), c, y), ys)
        else:
            for dy in range(1, ny):
                take(p, rep_of(q, c, back_y(dy)), xs)

    def near_rest(p):
        if pieces[p][3] == 0:
            for dy in range(1, ny):
                take(p, rep_of(q, c, back_y(dy)), [])
        else:
            for dq in range(1, nq):
                take(p, rep_of(back_q(dq), c, y), [])

    def far(p):
        for dq in range(1, nq):
            for dy in range(1, ny):
                take(p, rep_of(back_q(dq), c, back_y(dy)), [])

    def from_partner(p):
        for dq in range(nq):
            for dy in range(ny):
                rep = rep_of(at_q(dq), 1 - c, at_y(dy))
                arrived(slot(p, rep), w_sem.at[p * peers * 2 + rep])

    always = col >= 0
    chain(0, 1, always, always)
    if n_col == 4:
        own_features(1, middle & low, middle & high)
    for p in early:
        near_first(p)
    for p in later:
        own_piece(p, xs)
    for p in reversed(later):
        own_piece(p, ys)
    for p in later:
        own_piece(p, [partner])
    for step in range(2, n_col - 1):
        chain(0, step, always, always)
    prompt = jnp.logical_not(late_mid)
    if n_col == 4:
        own_features(1, middle & high, middle & low, [0])
        own_features(1, middle & high & prompt, middle & low & prompt, [1])
        chain(1, 1, middle & low, middle & high)
    else:
        own_features(1, middle, middle)
    for p in early:
        near_rest(p)
    if n_col > 2:
        chain(0, n_col - 1, always, always)
    if n_col == 4:
        chain(1, 1, middle & high, middle & low)
    else:
        chain(1, 1, middle, middle)
    for p in early:
        far(p)
    for p in early:
        from_partner(p)
    for copy in locals_:
        copy.wait()

    mt, nt = tile_of(toks, 256), tile_of(hid, 384)
    m_tiles, n_tiles = toks // mt, hid // nt
    token_dims = (((0,), (0,)), ((), ()))

    def tile_slices(i):
        m, n = i // n_tiles, i % n_tiles
        return pl.ds(pl.multiple_of(m * mt, mt), mt), pl.ds(pl.multiple_of(n * nt, nt), nt)

    def project(first, last):
        @pl.loop(first, last)
        def _(i):
            ms, ns = tile_slices(i)
            x = full[0, :, ms]
            gate_pre = lax.dot_general(x, weights[0, :, ns], token_dims, preferred_element_type=F32)
            up_pre = lax.dot_general(x, weights[1, :, ns], token_dims, preferred_element_type=F32)
            act_val, slope_val = gelu_parts(gate_pre)
            grads[2, ms, ns] = (act_val * up_pre).astype(BF16)
            stash[0, ms, ns] = up_pre * slope_val
            stash[1, ms, ns] = act_val

    tiles = m_tiles * n_tiles
    project(0, tiles // 2)
    for p in later:
        near_first(p)
    for step in range(2, n_col - 1):
        chain(1, step, middle, middle)
    if staggered:
        own_features(1, middle & high & late_mid, middle & low & late_mid, [1])
    project(tiles // 2, tiles)

    def term(w, rep):
        return jnp.dot(full[w // 2, rows_at(rep, 0, rows), :], grads[w], preferred_element_type=F32)

    def pair_copy(i, spot=0):
        return pltpu.make_async_remote_copy(
            src_ref=partner_out.at[spot],
            dst_ref=sums.at[i],
            send_sem=pair_send.at[i],
            recv_sem=pair_recv.at[i],
            device_id=partner,
            device_id_type=MESH,
        )

    last_stage = max(n_col - 2, 0)

    def stage_of(rep, late):
        block = (rep * rows) // feats
        dist = jnp.abs(block - col)
        plain = jnp.where(at_end, jnp.maximum(dist - 1, 0), 0)
        if not staggered:
            return plain
        second_half = lax.rem(rep, feats // rows) == 1
        shifted = jnp.where(dist == 1, jnp.where(second_half, 2, 0), jnp.maximum(dist - 2, 0))
        return jnp.where(late, shifted, plain)

    def own_stage(rep):
        return stage_of(rep, late_end)

    def sum_stage(rep, route):
        return own_stage(rep)

    first_base, count = [], [0, 0]
    for w, _, _, route in pieces:
        first_base.append(count[w // 2])
        count[w // 2] += (nq - 1) * ny if route == 0 else (ny - 1) * nq
    second_base, count = [], [0, 0]
    for w, _, _, route in pieces:
        second_base.append(count[w // 2])
        count[w // 2] += (ny - 1) if route == 0 else (nq - 1)

    def first_slot(p, dq, dy):
        k = first_base[p] + ((dq - 1) * ny + dy if pieces[p][3] == 0 else (dy - 1) * nq + dq)
        late = pieces[p][0] // 2
        return first_in[late].at[k], first_sem[late].at[k]

    def second_slot(p, d):
        k = second_base[p] + d - 1
        late = pieces[p][0] // 2
        return second_in[late].at[k], second_sem[late].at[k]

    def partner_term(w, dq, dy, when=None, ahead=False):
        rep = rep_of(at_q(dq), 1 - c, at_y(dy))
        i = w * peers + at_q(dq) * ny + at_y(dy)

        def one():
            spot = 2 * peers if ahead else lax.rem(i, 2 * peers)
            if w == 0 and not ahead:
                pair_copy(2 * peers + i).wait_send()
            partner_out[spot] = term(w, rep).astype(BF16)
            pair_copy(i, spot).start()

        guarded(None if when is None else when(rep), one)

    def slice_copy(p, dq, dy):
        w, r0, nr, route = pieces[p]
        index = w * peers + at_q(dq) * ny + at_y(dy)
        dst, sem = first_slot(p, dq, dy)
        return pltpu.make_async_remote_copy(
            src_ref=sums.at[index, pl.ds(r0, nr), :],
            dst_ref=dst,
            send_sem=slice_sem.at[p * peers + dq * ny + dy],
            recv_sem=sem,
            device_id=q_peer(dq) if route == 0 else y_peer(dy),
            device_id_type=MESH,
        )

    def own_term(w, dq, dy, when=None):
        index = w * peers + at_q(dq) * ny + at_y(dy)
        rep = rep_of(at_q(dq), c, at_y(dy))

        def one():
            arrived(sums.at[index], pair_recv.at[index])
            sums[index] = (term(w, rep) + sums[index].astype(F32)).astype(BF16)
            for p, (pw, _, _, route) in enumerate(pieces):
                if pw == w:
                    away = dq if route == 0 else dy
                    if not isinstance(away, int):
                        pl.when(away > 0)(slice_copy(p, dq, dy).start)
                    elif away:
                        slice_copy(p, dq, dy).start()

        guarded(None if when is None else when(rep), one)

    grid_order = [(dq, dy) for dq in others_first(nq) for dy in others_first(ny)]

    def place(i):
        return lax.rem(1 + i // ny, nq), lax.rem(1 + i % ny, ny)

    def partner_terms(w, when=None):
        @pl.loop(0, peers)
        def _(i):
            partner_term(w, *place(i), when)

    def own_terms(w, when=None):
        @pl.loop(0, peers)
        def _(i):
            own_term(w, *place(i), when)

    def second_send(p, when=None):
        w, r0, nr, route = pieces[p]
        rs = pl.ds(r0, nr)
        n_first, n_second = (nq, ny) if route == 0 else (ny, nq)
        for d in range(1, n_second):
            index = w * peers + (q * ny + at_y(d) if route == 0 else at_q(d) * ny + y)
            rep = rep_of(q, c, at_y(d)) if route == 0 else rep_of(at_q(d), c, y)
            cond = None if when is None else when(sum_stage(rep, route))

            def one():
                total = sums[index, rs, :].astype(F32)
                for f in range(1, n_first):
                    ref, sem = first_slot(p, f, d) if route == 0 else first_slot(p, d, f)
                    arrived(ref, sem)
                    total = total + ref[...].astype(F32)
                sums[index, rs, :] = total.astype(BF16)

            guarded(cond, one)
            dst, sem = second_slot(p, d)
            where = y_peer(d) if route == 0 else q_peer(d)
            sends.start(sums.at[index, rs, :], dst, sem, where, cond, ("sum", p, d))

    outs = (og_ref, ou_ref, od_ref)
    scale = 1.0 / math.sqrt(toks * n_dp * n_row)

    def second_own(p):
        w, r0, nr, route = pieces[p]
        rs = pl.ds(r0, nr)
        total = sums[w * peers + q * ny + y, rs, :].astype(F32)
        for f in range(1, nq if route == 0 else ny):
            ref, sem = first_slot(p, f, 0) if route == 0 else first_slot(p, 0, f)
            arrived(ref, sem)
            total = total + ref[...].astype(F32)
        outs[w][rs, :] = total * scale

    def second_final(p):
        w, r0, nr, route = pieces[p]
        rs = pl.ds(r0, nr)
        for d in range(1, ny if route == 0 else nq):
            ref, sem = second_slot(p, d)
            arrived(ref, sem)
            outs[w][rs, :] = outs[w][rs, :] + ref[...].astype(F32) * scale

    at_block = lambda when_low, when_high: jnp.where(low, when_low, when_high) * feats
    if staggered:
        spans = [
            [(at_block(0, 3), feats), (at_block(2, 1), feats)],
            [(at_block(3, 0), feats), (at_block(1, 2), half)],
            [(at_block(1, 2) + half, half)],
        ]
    else:
        spans = [[(at_block(0, n_col - 1), feats)], [], [(at_block(n_col - 1, 0), feats)]]
        if n_col > 2:
            spans[1].append((feats + 0 * col, (n_col - 2) * feats))

    def hidden_grad_over(phase):
        if not spans[phase]:
            return

        @pl.loop(0, m_tiles)
        def _(m):
            ms = pl.ds(pl.multiple_of(m * mt, mt), mt)
            part = None if phase == 0 else acc[ms, :]
            for start, size in spans[phase]:
                ks = pl.ds(pl.multiple_of(start, 16), size)
                more = lax.dot_general(full[1, ks, ms], weights[2, ks, :], token_dims, preferred_element_type=F32)
                part = more if part is None else part + more
            acc[ms, :] = part

    stage_is = lambda k: lambda rep: own_stage(rep) == k
    on_time = jnp.logical_not(late_end)
    for k in range(last_stage):
        if k == 0:
            end_wait(1, range(2), on_time)
            if staggered:
                end_wait(1, [0], late_end)
                end_wait(2, range(2), late_end)
        else:
            end_wait(k + 1, range(2), on_time)
            if staggered:
                end_wait(k + 2, range(2), late_end)
        partner_terms(2, stage_is(k))
        if k == last_stage - 1 and k > 0:
            for p in later:
                second_send(p, lambda k: k < last_stage - 1)
            hidden_grad_over(1)
        own_terms(2, stage_is(k))
        if k == 0:
            for p in later:
                near_rest(p)
            for p in later:
                far(p)
            for p in later:
                from_partner(p)
            hidden_grad_over(0)

    end_wait(n_col - 1, range(2), on_time)
    if staggered:
        end_wait(1, [1], late_end)
    hidden_grad_over(2)
    et = tile_of(toks, 32)

    def finish_grad(w):
        @pl.loop(0, toks // et)
        def _(m):
            ms = pl.ds(pl.multiple_of(m * et, et), et)
            grads[w, ms, :] = (acc[ms, :] * stash[w, ms, :]).astype(BF16)

    rt = tile_of(feats, 288)
    hid_dims = (((1,), (1,)), ((), ()))

    def ig_slot(going_left, d, h):
        k = (going_left * n_col + d) * 2 + h
        return ig_in.at[going_left * (n_col - 1) + d - (1 - going_left), pl.ds(h * half, half), :], ig_sem.at[k]

    def input_part(k):
        block = jnp.where(low, n_col - 1 - k, k)

        @pl.loop(0, feats // rt)
        def _(r):
            rs = pl.ds(pl.multiple_of(block * feats + r * rt, 8), rt)
            part = lax.dot_general(weights[0, rs, :], grads[0], hid_dims, preferred_element_type=F32)
            part = part + lax.dot_general(weights[1, rs, :], grads[1], hid_dims, preferred_element_type=F32)
            ig_out[block, pl.ds(pl.multiple_of(r * rt, 8), rt), :] = part.astype(BF16)

        if k < n_col - 1:
            for h in range(2):
                src = lambda b: ig_out.at[b, pl.ds(h * half, half), :]
                dst, sem = ig_slot(0, n_col - 1 - k, h)
                sends.start(src(n_col - 1 - k), dst, sem, right, col == 0, ("part", k, h))
                dst, sem = ig_slot(1, k, h)
                sends.start(src(k), dst, sem, left, col == n_col - 1, ("part", k, h))

    def relay(going_left, k, side=None):
        d = k if going_left else n_col - 1 - k
        inside = (col > d) & (col < n_col - 1) if going_left else (col < d) & (col > 0)
        if side is not None:
            inside = inside & side
        for h in range(2):
            ref, sem = ig_slot(going_left, d, h)
            part = ig_out.at[d, pl.ds(h * half, half), :]

            def one():
                arrived(ref, sem)
                part[...] = (part[...].astype(F32) + ref[...].astype(F32)).astype(BF16)

            guarded(inside, one)
            where = left if going_left else right
            sends.start(part, ref, sem, where, inside, ("relay", going_left, k, h))

    sent = [[g for g in grid_order if g[0]], [g for g in grid_order if g[1]]]
    for i in range(max(len(sent[0]), len(sent[1]))):
        both = [(w, sent[w][i]) for w in range(2) if i < len(sent[w])]
        for w, place_i in both:
            if i == 0:
                finish_grad(w)
            partner_term(w, *place_i, ahead=w == 0 and i == 0)
        if i == 0:
            partner_terms(2, stage_is(last_stage))
        for w, place_i in both:
            own_term(w, *place_i)
        if i == 0:
            own_terms(2, stage_is(last_stage))
            for p in later:
                second_send(p, lambda k: k == last_stage - 1)
            input_part(0)
    for p in later:
        second_send(p, lambda k: k == last_stage)
    for k in range(1, n_col - 1):
        input_part(k)
    for w in range(2):
        @pl.loop(0, peers // (nq if w == 0 else ny))
        def _(i):
            j = lax.rem(i + 1, ny if w == 0 else nq)
            partner_term(w, *((0, j) if w == 0 else (j, 0)))

        @pl.loop(0, peers // (nq if w == 0 else ny))
        def _(i):
            j = lax.rem(i + 1, ny if w == 0 else nq)
            own_term(w, *((0, j) if w == 0 else (j, 0)))

    input_part(n_col - 1)
    relay(0, 0, low)
    relay(1, 0, high)
    for p in early:
        second_send(p)
    for k in range(1, n_col - 1):
        relay(0, k, low)
        relay(1, k, high)
    for k in range(n_col - 1):
        relay(1, k, low)
        relay(0, k, high)
    for p in early:
        second_own(p)
    for p in later:
        second_own(p)
    for p in later:
        second_final(p)

    for h in range(2):
        hs = pl.ds(h * half, half)
        from_left, left_sem = ig_slot(0, jnp.maximum(col, 1), h)
        from_right, right_sem = ig_slot(1, jnp.minimum(col, n_col - 2), h)
        guarded(has_left, lambda: arrived(from_left, left_sem))
        guarded(has_right, lambda: arrived(from_right, right_sem))
        own = ig_out[col, hs, :].astype(F32)

        @pl.when(has_left & has_right)
        def _():
            ig_ref[hs, :] = (own + from_left[...].astype(F32) + from_right[...].astype(F32)).astype(BF16)

        @pl.when(jnp.logical_not(has_left))
        def _():
            ig_ref[hs, :] = (own + from_right[...].astype(F32)).astype(BF16)

        @pl.when(jnp.logical_not(has_right))
        def _():
            ig_ref[hs, :] = (own + from_left[...].astype(F32)).astype(BF16)

    for p in early:
        second_final(p)
    sends.finish()

    dq, dy = sent[0][0]
    pair_copy(2 * peers + at_q(dq) * ny + at_y(dy)).wait_send()

    @pl.loop(0, 2 * peers)
    def _(i):
        pair_copy(i).wait_send()

    for p, (_, _, _, route) in enumerate(pieces):
        @pl.loop(0, peers)
        def _(i):
            dq, dy = i // ny, i % ny
            pl.when((dq if route == 0 else dy) > 0)(slice_copy(p, dq, dy).wait_send)


def flush(parts, *refs):
    sems = refs[8]
    copies = []
    for i in range(4):
        src, dst = refs[i], refs[4 + i]
        pieces = next(n for n in range(parts, 0, -1) if n == 1 or src.shape[0] % (16 * n) == 0)
        step = src.shape[0] // pieces
        for j in range(pieces):
            at = pl.ds(j * step, step)
            copies.append(pltpu.make_async_copy(src.at[at, :], dst.at[at, :], sems.at[i * parts + j]))
            copies[-1].start()
    for copy in copies:
        copy.wait()


def body(n_dp, n_row, n_col, act_in, cot_out, w_gate, w_up, w_down):
    toks, feats = act_in.shape
    rows, hid = w_gate.shape
    sizes = (n_dp, n_row, n_col, rows, hid, feats, toks)
    nq, ny = n_dp // 2, n_row
    peers, reps, dim = nq * ny, n_dp * n_row, feats * n_col
    pieces = pieces_of(rows)
    firsts, seconds = [0, 0], [0, 0]
    for w, _, _, route in pieces:
        firsts[w // 2] += (nq - 1) * ny if route == 0 else (ny - 1) * nq
        seconds[w // 2] += (ny - 1) if route == 0 else (nq - 1)
    n_pieces = len(pieces)
    n_sends = 8 + 8 * (n_col - 2)
    n_sends += n_pieces * (nq + ny - 1)
    for _, _, _, route in pieces:
        n_sends += (nq - 1) * ny + ny - 1 if route == 0 else (ny - 1) * nq + nq - 1
        n_sends += (nq - 1) * (ny - 1)
    n_sends += sum(seconds) + 6 * (n_col - 1)
    late_rows = min(nr for w, _, nr, _ in pieces if w == 2)
    any_spec = pl.BlockSpec(memory_space=pl.ANY)
    dma = lambda n: pltpu.SemaphoreType.DMA((max(n, 1),))
    landing = lambda n: [pltpu.VMEM((max(n[0], 1), rows, hid), BF16), pltpu.VMEM((max(n[1], 1), late_rows, hid), BF16)]
    wgrad = pltpu.VMEM((rows, hid), F32)
    ig_t, gate_grad, up_grad, down_t = pl.pallas_call(
        functools.partial(kernel, sizes),
        out_shape=[pltpu.VMEM((feats, toks), BF16), wgrad, wgrad, wgrad],
        in_specs=[any_spec] * 5,
        out_specs=[pl.BlockSpec(memory_space=pltpu.VMEM)] * 4,
        scratch_shapes=[
            pltpu.VMEM((2, dim, toks), BF16),
            pltpu.VMEM((3, dim, hid), BF16),
            pltpu.VMEM((3, toks, hid), BF16),
            pltpu.VMEM((2, toks, hid), F32),
            pltpu.VMEM((toks, hid), F32),
            pltpu.VMEM((2 * peers + 1, rows, hid), BF16),
            pltpu.VMEM((3 * peers, rows, hid), BF16),
            landing(firsts),
            landing(seconds),
            pltpu.VMEM((n_col, feats, toks), BF16),
            pltpu.VMEM((2 * (n_col - 1), feats, toks), BF16),
            dma(5), dma(n_sends), dma(n_pieces * reps), dma(4 * n_col), dma(3 * peers), dma(3 * peers),
            [dma(n) for n in firsts], [dma(n) for n in seconds], dma(4 * n_col),
            dma(n_pieces * peers),
        ],
        compiler_params=pltpu.CompilerParams(
            collective_id=0, has_side_effects=True, vmem_limit_bytes=61400000
        ),
    )(act_in.T, cot_out.T, w_gate, w_up, w_down.T)
    parts = 4
    ig_t, gate_grad, up_grad, down_t = pl.pallas_call(
        functools.partial(flush, parts),
        out_shape=[jax.ShapeDtypeStruct((feats, toks), BF16)] + [jax.ShapeDtypeStruct((rows, hid), F32)] * 3,
        in_specs=[pl.BlockSpec(memory_space=pltpu.VMEM)] * 4,
        out_specs=[any_spec] * 4,
        scratch_shapes=[dma(4 * parts)],
        compiler_params=pltpu.CompilerParams(vmem_limit_bytes=1 << 20),
    )(ig_t, gate_grad, up_grad, down_t)
    return (ig_t.T, gate_grad, up_grad, down_t.T)


def solution(mesh):
    grid = P(("dp", "row"), "col")
    flipped = P("col", ("dp", "row"))
    return jax.shard_map(
        functools.partial(body, mesh.shape["dp"], mesh.shape["row"], mesh.shape["col"]),
        mesh=mesh,
        in_specs=(grid, grid, grid, grid, flipped),
        out_specs=(grid, grid, grid, flipped),
        check_vma=False,
    )
```
